32 devices in a mesh: blk: 16 (over z, y, core), grp: 2 (over x).
Axes of the slice: x: 2, y: 2, z: 4, core: 2. Of those that a mesh axis runs over, the one named last changes fastest.
Arguments:
- integrals: bfloat16 [64, 512, 1024], P('blk', None, 'grp'), may hold values from -1.1953125 to 1.1953125
- eps_occ: float32 [64], replicated, may hold values from -2 to -0.5
- eps_vir: float32 [512], replicated, may hold values from 0.3 to 3
- pair_mask: int32 [64, 4, 4], P('blk'), may hold values 0 or 1
Outputs:
- density: float32 [64, 512, 1024], P('blk', 'grp')
The draws below stay inside these ranges and needn't reach their ends.
All inputs are finite; a program needn't handle non-finite values. No bound on the sum of `pair_mask` on one device may be relied on, other than what follows from the above.
Results may differ from the reference program's by a relative error of at most 0.0035.
Values may be sent and summed in bfloat16 or wider, within the bound.
No kernel may reach another device: no remote copies, remote signals or barrier semaphores. Data moves between devices by JAX's collectives and lax.ppermute only.
A program may use at most 128 MiB of HBM per device.

```python
import jax
import jax.numpy as jnp
from jax import lax

NVIR = 512
NAUX = 1024
OCC_DEV = 4
SHIFTS = 4
NOCC = 64
SLAB = 256
N_GRP = 2


def set_ends(drawn, stream_key, low, high):
    shape = drawn.shape
    place = [jax.random.randint(jax.random.fold_in(stream_key, axis), (), 0, shape[axis]) for axis in range(len(shape))]
    drawn = drawn.at[tuple(place)].set(low)
    longest = shape.index(max(shape))
    place[longest] = (place[longest] + 1) % shape[longest]
    return drawn.at[tuple(place)].set(high)


def levels(stream_key, shape, cuts, least, top_value):
    loudness, own = 1.0, jax.random.fold_in(stream_key, 6)
    for dim, blocks in cuts:
        heights = jnp.exp(jax.random.uniform(jax.random.fold_in(own, dim), (blocks,), jnp.float32, least / len(cuts), top_value / len(cuts)))
        loudness = loudness * jnp.repeat(heights, shape[dim] // blocks).reshape([-1 if axis == dim else 1 for axis in range(len(shape))])
    return loudness


def bell_draw(rng, dims, width, limit, shards=(), kind=jnp.bfloat16):
    array = jax.random.normal(rng, dims, jnp.float32) * width
    if len(shards) > 0:
        array = levels(rng, dims, shards, -0.22, 0.18) * array
    return jnp.clip(array, min=-limit, max=limit).astype(kind)


def setup_inputs(seed: int = 0) -> dict:
    streams_of = jax.random.split(jax.random.key(seed), 5)
    return {
        "integrals": bell_draw(streams_of[0], (NOCC, NVIR, NAUX), 0.18, 1.1953125, ((0, 16), (2, 2))),
        "eps_occ": jnp.clip(jax.random.uniform(streams_of[1], (NOCC,), jnp.float32, -2.0, -0.5), -2.0, -0.5),
        "eps_vir": jnp.clip(jax.random.uniform(streams_of[2], (NVIR,), jnp.float32, 0.3, 3.0), 0.3, 3.0),
        "pair_mask": set_ends((jax.random.randint(streams_of[3], (NOCC, SHIFTS, OCC_DEV), 0, 4) < 3).astype(jnp.int32), jax.random.fold_in(streams_of[3], 1), 0, 1),
    }


def reference(integrals, eps_occ, eps_vir, pair_mask):
    nblk = NOCC // OCC_DEV
    blocks = integrals.astype(jnp.float32).reshape(nblk, OCC_DEV, NVIR, NAUX)
    energies = eps_occ.reshape(nblk, OCC_DEV)
    masks = pair_mask.astype(jnp.float32).reshape(nblk, OCC_DEV, SHIFTS, OCC_DEV)
    density = jnp.zeros((nblk, OCC_DEV, NVIR, NAUX), jnp.float32)
    for shift in range(1, SHIFTS + 1):
        partner_blocks = jnp.roll(blocks, shift, axis=0)
        partner_energy = jnp.roll(energies, shift, axis=0)
        weights = masks[:, :, shift - 1, :]

        def one_block(items):
            left, right, left_e, right_e, weight = items
            coulomb = jnp.einsum("oap,lbp->olab", left, right)
            denom = left_e[:, None, None, None] + right_e[None, :, None, None] - eps_vir[None, None, :, None] - eps_vir[None, None, None, :]
            amplitude = (weight[:, :, None, None] * coulomb / denom).astype(jnp.bfloat16).astype(jnp.float32)
            own_part = jnp.einsum("olab,lbp->oap", amplitude, right)
            split_amp = amplitude.reshape(OCC_DEV, OCC_DEV, N_GRP, SLAB, NVIR)
            split_left = left.reshape(OCC_DEV, N_GRP, SLAB, NAUX)
            pieces = jnp.einsum("olgab,ogap->glbp", split_amp, split_left)
            pieces = lax.optimization_barrier(pieces.astype(jnp.bfloat16)).astype(jnp.float32)
            return own_part, jnp.sum(pieces, axis=0)

        own_part, partner_part = lax.map(one_block, (blocks, partner_blocks, energies, partner_energy, weights))
        density = density + own_part + jnp.roll(partner_part, -shift, axis=0)
    return density.reshape(NOCC, NVIR, NAUX)
```

```python
import functools

import jax
import jax.numpy as jnp
from jax import lax
from jax.experimental import pallas as pl
from jax.experimental.pallas import tpu as pltpu
from jax.sharding import PartitionSpec as P


LAST = (((1,), (1,)), ((), ()))
CHUNK = 512
TILE = 16


def flipped(block, bit):
    return lax.ppermute(block, "blk", [(i ^ bit, i) for i in range(lax.axis_size("blk"))])


def sorted_out(block, distance):
    size = lax.axis_size("blk")
    route = [((i - distance if i & 2 else i + distance) % size, i) for i in range(size)]
    return lax.ppermute(block, "blk", route)


def turned(block, distance):
    size = lax.axis_size("grp")
    return lax.ppermute(block, "grp", [(i, (i + distance) % size) for i in range(size)])


def terms_body(names, count, parts, rows, shifts, chunk, carried, scalars, *refs):
    refs = list(refs)
    left = [refs.pop(0) for _ in range(parts)]
    right = [[refs.pop(0) for _ in range(parts)] for _ in range(count)]
    flag_ref, col_ref, row_ref = refs.pop(0), refs.pop(0), refs.pop(0)
    base_ref = refs.pop(0) if carried else None
    out_ref, amp_ref = refs
    _, width = left[0].shape[1:]
    occ, nvir = names["occ"], names["nvir"]
    o = pl.program_id(1) + names["first_occ"]
    col = col_ref[0]
    lane = lax.broadcasted_iota(jnp.int32, (1, width), 1)
    flags = flag_ref[0:TILE, :].astype(jnp.float32)[0:1]
    for n in range(count):
        step = scalars[names["steps"] + n]
        theirs = right[n][0][rows : rows + TILE, :].astype(jnp.float32)[0:1]
        source = jnp.where(step > 0, theirs, flags)
        for start in range(0, rows, chunk):
            cut = slice(start, start + chunk)
            other = (scalars[names["start"]] + start) // nvir
            place = jnp.where(step > 0, (other * shifts + step - 1) * occ + o, (o * shifts - step - 1) * occ + other)
            weight = jnp.sum(jnp.where(lane == place, source, 0.0), axis=1, keepdims=True)
            coulomb = None
            for p in range(parts):
                piece = lax.dot_general(left[p][0], right[n][p][cut, :], LAST, preferred_element_type=jnp.float32)
                coulomb = piece if coulomb is None else coulomb + piece
            denom = col + row_ref[n, :, cut]
            amp_ref[:, n * rows + start : n * rows + start + chunk] = (weight * coulomb / denom).astype(jnp.bfloat16)
    for p in range(parts):
        at = pl.ds(pl.multiple_of(scalars[p], 128), width)
        total = base_ref[0, 0, :, at] if carried else None
        for n in range(count):
            piece = jnp.dot(
                amp_ref[:, n * rows : (n + 1) * rows], right[n][p][0:rows, :], preferred_element_type=jnp.float32
            )
            total = piece if total is None else total + piece
        out_ref[0, 0, :, at] = total.astype(out_ref.dtype)


def terms(own, right, first, base, slabs, occs, dtype=jnp.float32):
    left, places = own["left"], own["places"]
    count, parts = len(right), len(left)
    occ, nvir, width = left[0].shape
    rows = own["rows"]
    naux = width * parts
    slab = nvir // lax.axis_size("grp")
    first_slab, first_occ = slabs[0], occs[0]
    out = (slabs[1], occs[1], slab, naux)
    block = (1, 1, slab, naux)

    def at_left(p):
        return lambda j, o, s: ((o + first_occ + s[places["turn"] + p]) % occ, s[places["slab"] + j + first_slab], 0)

    in_specs = [pl.BlockSpec((1, slab, width), at_left(p)) for p in range(parts)]
    in_specs += [pl.BlockSpec(piece.shape, lambda j, o, s: (0, 0)) for pieces in right for piece in pieces]
    in_specs += [
        pl.BlockSpec(own["flags"].shape, lambda j, o, s: (0, 0)),
        pl.BlockSpec((1, slab, 1), lambda j, o, s: (o + first_occ, s[places["slab"] + j + first_slab], 0)),
        pl.BlockSpec((count, 1, rows), lambda j, o, s: (0, 0, 0)),
    ]
    row = own["row"][first : first + count]
    args = [*left, *[piece for pieces in right for piece in pieces], own["flags"], own["col"], row]
    if base is not None:
        skip = first_slab - base[1]
        in_specs.append(pl.BlockSpec(block, lambda j, o, s: (j + skip, o + first_occ, 0, 0)))
        args.append(base[0])
    moved = sum(p.size * 2 for pieces in right for p in pieces) + out[0] * out[1] * slab * naux * 10
    names = {"occ": occ, "nvir": nvir, "first_occ": first_occ, "steps": places["steps"] + first, "start": places["start"]}
    return pl.pallas_call(
        functools.partial(
            terms_body, names, count, parts, rows, own["shifts"], min(CHUNK, rows, nvir), base is not None
        ),
        grid_spec=pltpu.PrefetchScalarGridSpec(
            num_scalar_prefetch=1,
            grid=(slabs[1], occs[1]),
            in_specs=in_specs,
            out_specs=pl.BlockSpec(block, lambda j, o, s: (j, o, 0, 0)),
            scratch_shapes=[pltpu.VMEM((slab, count * rows), jnp.bfloat16)],
        ),
        out_shape=jax.ShapeDtypeStruct(out, dtype),
        compiler_params=pltpu.CompilerParams(
            dimension_semantics=("arbitrary", "arbitrary"), vmem_limit_bytes=56 * 2**20
        ),
        cost_estimate=pl.CostEstimate(
            flops=4 * out[0] * out[1] * slab * rows * count * naux, bytes_accessed=moved, transcendentals=0
        ),
        name="terms",
    )(own["scalars"], *args)


def shards(integrals, eps_occ, eps_vir, pair_mask):
    occ, nvir, width = integrals.shape
    shifts = pair_mask.shape[1]
    groups = lax.axis_size("grp")
    cycle = lax.axis_size("blk")
    assert shifts == 4 and cycle % 4 == 0
    rank = lax.axis_index("grp")
    place = lax.axis_index("blk")
    core, side = place & 1, (place >> 1) & 1
    every = occ * nvir
    rows = every // groups
    start = rank * rows

    up_core, up_side = 1 - 2 * core, 1 - 2 * side
    diag = -2 * up_side
    steps = [up_core, 2 * up_side, 2 * up_side + up_core, 4 * up_side, -4 * up_side, -3 * up_core, diag, diag + up_core]
    energy = eps_occ.reshape(cycle, occ)
    row = (energy[(place + jnp.stack(steps)) % cycle][:, :, None] - eps_vir).reshape(-1, 1, every)
    row = lax.dynamic_slice_in_dim(row, start, rows, 2)
    col = (energy[place][:, None] - eps_vir)[:, :, None]

    flat = integrals.reshape(every, width)
    if groups == 2 and occ % 2 == 0:
        per = occ // groups
        flags = jnp.pad(pair_mask.astype(integrals.dtype).reshape(1, -1), ((0, TILE - 1), (0, width - pair_mask.size)))
        ahead = turned(lax.dynamic_slice_in_dim(flat, (1 - rank) * rows, rows, 0), 1)
        mine = [jnp.concatenate([lax.dynamic_slice_in_dim(flat, start, rows, 0), flags]), ahead]
        rest = turned(mine[0], 1)
        joined = jnp.concatenate([ahead, rest[:rows]])
        left = [integrals, joined.reshape(integrals.shape)]
        offsets = [rank * width, (1 - rank) * width]
        turns = [0 * rank, (groups - rank) * per]
    else:
        left = [lax.all_gather(integrals, "grp", axis=2, tiled=True)]
        naux = left[0].shape[2]
        flags = jnp.pad(pair_mask.astype(integrals.dtype).reshape(1, -1), ((0, TILE - 1), (0, naux - pair_mask.size)))
        mine = [jnp.concatenate([lax.dynamic_slice_in_dim(left[0].reshape(every, naux), start, rows, 0), flags])]
        offsets, turns = [0 * rank], [0 * rank]
    slabs = [(rank + 1 + j) % groups for j in range(groups)]
    parts = len(left)
    scalars = jnp.stack([*offsets, *turns, *slabs, start, *steps]).astype(jnp.int32)
    places = {"turn": parts, "slab": 2 * parts, "start": 2 * parts + groups, "steps": 2 * parts + groups + 1}
    own = {
        "left": left, "flags": flags, "col": col, "row": row, "scalars": scalars, "places": places, "rows": rows,
        "shifts": shifts,
    }

    def each(pieces, move):
        out = []
        for piece in pieces:
            out.append(move(piece))
        return out

    def mixed(first, second):
        return [jnp.where(core == side, a, b) for a, b in zip(first, second)]

    everything, both = (0, occ), (0, groups)
    last = groups - 1
    near = each(mine, lambda x: flipped(x, 2))
    fore = each(mine, lambda x: sorted_out(x, 4))
    sibling = each(mine, lambda x: flipped(x, 1))
    cross = each(near, lambda x: flipped(x, 1))
    *mine, fore[-1] = lax.optimization_barrier((*mine, fore[-1]))
    across = each(fore, lambda x: flipped(x, 2))
    aft = each(mine, lambda x: sorted_out(x, -4))
    total = terms(own, [sibling, near], 0, None, both, everything)
    if parts > 1:
        total, across[0], aft[0] = lax.optimization_barrier((total, across[0], aft[0]))
    beyond = each(across[: parts - 1], lambda x: flipped(x, 1))
    far = each(mixed(fore[: parts - 1], aft), lambda x: flipped(x, 1))
    total = terms(own, [cross, fore], 2, (total, 0), both, everything)
    total, across[-1], aft[-1] = lax.optimization_barrier((total, across[-1], aft[-1]))
    beyond += each(across[-1:], lambda x: flipped(x, 1))
    far += each(mixed(fore[-1:], aft[-1:]), lambda x: flipped(x, 1))
    late = [aft, far, across, beyond]
    arrived = []
    at = 0
    for size in cuts(occ):
        out = terms(own, late, 4, (total, 0), (0, last), (at, size), jnp.bfloat16)
        arrived.append((at, size, [turned(out[d - 1], d) for d in range(1, groups)]))
        at += size
    total, _ = lax.optimization_barrier((total, out))
    kept = terms(own, late, 4, (total, 0), (last, 1), everything)[0]
    for at, size, pieces in arrived:
        kept = kept.at[at : at + size].add(sum(piece.astype(jnp.float32) for piece in pieces))
    return kept


def cuts(count):
    return [1, 1, count - 2] if count > 2 else [1] * count


def solution(mesh):
    placed = (P("blk", None, "grp"), P(), P(), P("blk", None, None))
    return jax.shard_map(shards, mesh=mesh, in_specs=placed, out_specs=P("blk", "grp", None), check_vma=False)
```

```python
import functools

import jax
import jax.numpy as jnp
from jax import lax
from jax.experimental import pallas as pl
from jax.experimental.pallas import tpu as pltpu
from jax.sharding import PartitionSpec as P


LAST = (((1,), (1,)), ((), ()))
CHUNK = 512
GRANT = 20 * 2**20
TILE = 16


def flipped(block, bit):
    return lax.ppermute(block, "blk", [(i ^ bit, i) for i in range(lax.axis_size("blk"))])


def sorted_out(block, distance):
    size = lax.axis_size("blk")
    route = [((i - distance if i & 2 else i + distance) % size, i) for i in range(size)]
    return lax.ppermute(block, "blk", route)


def turned(block, distance):
    size = lax.axis_size("grp")
    return lax.ppermute(block, "grp", [(i, (i + distance) % size) for i in range(size)])


def terms_body(names, layout, parts, rows, chunk, adds, carried, scalars, *refs):
    refs = list(refs)
    shifts, occ, nvir = names["shifts"], names["occ"], names["nvir"]
    count = len(layout)
    o = pl.program_id(1) + names["first_occ"]
    left = [refs.pop(0)[0]]
    if parts > 1:
        ahead, rest = refs.pop(0), refs.pop(0)
        left.append(jnp.where((o + scalars[names["turn"]]) % occ < names["per"], ahead[...], rest[...]))
    right = [[[refs.pop(0) for _ in range(parts)] for _ in range(options)] for options in layout]
    flag_ref, col_ref, row_ref = refs.pop(0), refs.pop(0), refs.pop(0)
    base_ref = refs.pop(0) if carried else None
    extra = [refs.pop(0) for _ in adds]
    out_ref, amp_ref, *chosen = refs
    for n, options in enumerate(layout):
        if options > 1:
            @pl.when((pl.program_id(0) == 0) & (pl.program_id(1) == 0))
            def pick():
                for p in range(parts):
                    chosen[p][...] = jnp.where(scalars[names["pick"]] == 0, right[n][0][p][...], right[n][1][p][...])

            right[n] = chosen
        else:
            right[n] = right[n][0]
    width = left[0].shape[1]
    col = col_ref[0]
    lane = lax.broadcasted_iota(jnp.int32, (1, width), 1)
    flags = flag_ref[0:TILE, :].astype(jnp.float32)[0:1]
    for n in range(count):
        step = scalars[names["steps"] + n]
        theirs = right[n][0][rows : rows + TILE, :].astype(jnp.float32)[0:1]
        source = jnp.where(step > 0, theirs, flags)
        for start in range(0, rows, chunk):
            cut = slice(start, start + chunk)
            other = (scalars[names["start"]] + start) // nvir
            place = jnp.where(step > 0, (other * shifts + step - 1) * occ + o, (o * shifts - step - 1) * occ + other)
            weight = jnp.sum(jnp.where(lane == place, source, 0.0), axis=1, keepdims=True)
            coulomb = None
            for p in range(parts):
                piece = lax.dot_general(left[p], right[n][p][cut, :], LAST, preferred_element_type=jnp.float32)
                coulomb = piece if coulomb is None else coulomb + piece
            denom = col + row_ref[n, :, cut]
            amp_ref[:, n * rows + start : n * rows + start + chunk] = (weight * coulomb / denom).astype(jnp.bfloat16)
    for p in range(parts):
        at = pl.ds(pl.multiple_of(scalars[p], 128), width)
        total = base_ref[0, 0, :, at] if carried else None
        for (begin, size), ref in zip(adds, extra):
            inside = (o >= begin) & (o < begin + size)
            total = total + jnp.where(inside, ref[0, :, at].astype(jnp.float32), 0.0)
        for n in range(count):
            piece = jnp.dot(
                amp_ref[:, n * rows : (n + 1) * rows], right[n][p][0:rows, :], preferred_element_type=jnp.float32
            )
            total = piece if total is None else total + piece
        out_ref[0, 0, :, at] = total.astype(out_ref.dtype)


def terms(own, right, first, base, slabs, occs, dtype=jnp.float32, arrived=(), in_hbm=False):
    left, places = own["left"], own["places"]
    parts = own["parts"]
    layout = [len(options) for options in right]
    count = len(layout)
    occ, nvir, width = left[0].shape
    rows = own["rows"]
    naux = width * parts
    slab = nvir // lax.axis_size("grp")
    first_slab, first_occ = slabs[0], occs[0]
    out = (slabs[1], occs[1], slab, naux)
    block = (1, 1, slab, naux)
    per = occ // parts

    def at_slab(j, s):
        return s[places["slab"] + j + first_slab]

    def at_part(taken):
        def at(j, o, s):
            turned_o = (o + first_occ + s[places["turn"]]) % occ - taken * per
            return jnp.clip(turned_o, 0, per - 1) * (nvir // slab) + at_slab(j, s), 0

        return at

    in_specs = [pl.BlockSpec((1, slab, width), lambda j, o, s: (o + first_occ, at_slab(j, s), 0))]
    in_specs += [pl.BlockSpec((slab, width), at_part(taken)) for taken in range(len(left) - 1)]
    pieces = [piece for options in right for option in options for piece in option]
    in_specs += [pl.BlockSpec(memory_space=pltpu.VMEM)] * len(pieces)
    in_specs += [
        pl.BlockSpec(own["flags"].shape, lambda j, o, s: (0, 0)),
        pl.BlockSpec((1, slab, 1), lambda j, o, s: (o + first_occ, at_slab(j, s), 0)),
        pl.BlockSpec((count, 1, rows), lambda j, o, s: (0, 0, 0)),
    ]
    args = [*left, *pieces, own["flags"], own["col"], own["row"][first : first + count]]
    if base is not None:
        skip = first_slab - base[1]
        in_specs.append(pl.BlockSpec(block, lambda j, o, s: (j + skip, o + first_occ, 0, 0)))
        args.append(pltpu.with_memory_space_constraint(base[0], pltpu.HBM))
    for begin, size, sums in arrived:
        in_specs.append(
            pl.BlockSpec(
                (1, slab, naux), lambda j, o, s, b=begin, z=size: (jnp.clip(o + first_occ - b, 0, z - 1), 0, 0)
            )
        )
        args.append(sums)
    moved = sum(piece.size * 2 for piece in pieces) + out[0] * out[1] * slab * naux * 10
    names = {
        "occ": occ, "nvir": nvir, "shifts": own["shifts"], "first_occ": first_occ, "per": per,
        "steps": places["steps"] + first, "start": places["start"], "turn": places["turn"], "pick": places["pick"],
    }
    scratch = [pltpu.VMEM((slab, count * rows), jnp.bfloat16)]
    if max(layout) > 1:
        scratch += [pltpu.VMEM(piece.shape, piece.dtype) for piece in right[layout.index(2)][0]]
    return pl.pallas_call(
        functools.partial(
            terms_body, names, layout, parts, rows, min(CHUNK, rows, nvir), [a[:2] for a in arrived], base is not None
        ),
        grid_spec=pltpu.PrefetchScalarGridSpec(
            num_scalar_prefetch=1,
            grid=(slabs[1], occs[1]),
            in_specs=in_specs,
            out_specs=pl.BlockSpec(block, lambda j, o, s: (j, o, 0, 0)),
            scratch_shapes=scratch,
        ),
        out_shape=pltpu.HBM(out, dtype) if in_hbm else jax.ShapeDtypeStruct(out, dtype),
        compiler_params=pltpu.CompilerParams(
            dimension_semantics=("arbitrary", "arbitrary"), vmem_limit_bytes=GRANT
        ),
        cost_estimate=pl.CostEstimate(
            flops=4 * out[0] * out[1] * slab * rows * count * naux, bytes_accessed=moved, transcendentals=0
        ),
        name="terms",
    )(own["scalars"], *args)


def settle_body(kept_ref, sums_ref, out_ref):
    out_ref[...] = kept_ref[...] + sums_ref[...].astype(jnp.float32)


def settle(kept, first, sums):
    block = (1, *kept.shape[1:])
    return pl.pallas_call(
        settle_body,
        grid=(sums.shape[0],),
        in_specs=[pl.BlockSpec(block, lambda o: (o + first, 0, 0)), pl.BlockSpec(block, lambda o: (o, 0, 0))],
        out_specs=pl.BlockSpec(block, lambda o: (o + first, 0, 0)),
        out_shape=jax.ShapeDtypeStruct(kept.shape, kept.dtype),
        input_output_aliases={0: 0},
        compiler_params=pltpu.CompilerParams(vmem_limit_bytes=GRANT),
        cost_estimate=pl.CostEstimate(flops=sums.size, bytes_accessed=10 * sums.size, transcendentals=0),
        name="settle",
    )(kept, sums)


def shards(integrals, eps_occ, eps_vir, pair_mask):
    occ, nvir, width = integrals.shape
    shifts = pair_mask.shape[1]
    groups = lax.axis_size("grp")
    cycle = lax.axis_size("blk")
    assert shifts == 4 and cycle % 4 == 0
    rank = lax.axis_index("grp")
    place = lax.axis_index("blk")
    core, side = place & 1, (place >> 1) & 1
    every = occ * nvir
    rows = every // groups
    start = rank * rows

    up_core, up_side = 1 - 2 * core, 1 - 2 * side
    diag = -2 * up_side
    steps = [up_core, 2 * up_side, 2 * up_side + up_core, 4 * up_side, -4 * up_side, -3 * up_core, diag, diag + up_core]
    energy = eps_occ.reshape(cycle, occ)
    row = (energy[(place + jnp.stack(steps)) % cycle][:, :, None] - eps_vir).reshape(-1, 1, every)
    row = lax.dynamic_slice_in_dim(row, start, rows, 2)
    col = (energy[place][:, None] - eps_vir)[:, :, None]

    flat = integrals.reshape(every, width)
    if groups == 2 and occ % 2 == 0:
        per = occ // groups
        flags = jnp.pad(pair_mask.astype(integrals.dtype).reshape(1, -1), ((0, TILE - 1), (0, width - pair_mask.size)))
        ahead = turned(lax.dynamic_slice_in_dim(flat, (1 - rank) * rows, rows, 0), 1)
        mine = [jnp.concatenate([lax.dynamic_slice_in_dim(flat, start, rows, 0), flags]), ahead]
        rest = turned(mine[0], 1)
        left = [integrals, ahead, rest]
        parts = 2
        offsets = [rank * width, (1 - rank) * width]
        turn = (groups - rank) * per
    else:
        left = [lax.all_gather(integrals, "grp", axis=2, tiled=True)]
        naux = left[0].shape[2]
        flags = jnp.pad(pair_mask.astype(integrals.dtype).reshape(1, -1), ((0, TILE - 1), (0, naux - pair_mask.size)))
        mine = [jnp.concatenate([lax.dynamic_slice_in_dim(left[0].reshape(every, naux), start, rows, 0), flags])]
        parts = 1
        offsets, turn = [0 * rank], 0 * rank
    slabs = [(rank + 1 + j) % groups for j in range(groups)]
    pick = jnp.where(core == side, 1, 0)
    scalars = jnp.stack([*offsets, turn, pick, start, *slabs, *steps]).astype(jnp.int32)
    places = {"turn": parts, "pick": parts + 1, "start": parts + 2, "slab": parts + 3, "steps": parts + 3 + groups}
    own = {
        "left": left, "flags": flags, "col": col, "row": row, "scalars": scalars, "places": places, "rows": rows,
        "shifts": shifts, "parts": parts,
    }

    def each(pieces, move):
        out = []
        for piece in pieces:
            out.append(move(piece))
        return out

    everything, both = (0, occ), (0, groups)
    last = groups - 1
    near = each(mine, lambda x: flipped(x, 2))
    fore = each(mine, lambda x: sorted_out(x, 4))
    sibling = each(mine, lambda x: flipped(x, 1))
    cross = each(near, lambda x: flipped(x, 1))
    aft = each(mine, lambda x: sorted_out(x, -4))
    across = each(fore, lambda x: flipped(x, 2))
    far_fore = each(fore, lambda x: flipped(x, 1))
    total = terms(own, [[sibling], [near]], 0, None, both, everything, in_hbm=True)
    if parts > 1:
        total, across[0], aft[0] = lax.optimization_barrier((total, across[0], aft[0]))
    beyond = each(across[: parts - 1], lambda x: flipped(x, 1))
    far_aft = each(aft[: parts - 1], lambda x: flipped(x, 1))
    sent = terms(own, [[cross], [fore]], 2, (total, 0), (0, last), everything, in_hbm=True)
    sent, across[-1], aft[-1] = lax.optimization_barrier((sent, across[-1], aft[-1]))
    beyond += each(across[-1:], lambda x: flipped(x, 1))
    far_aft += each(aft[-1:], lambda x: flipped(x, 1))
    late = [[aft], [far_fore, far_aft], [across], [beyond]]
    arrived = []
    at = 0
    for size in cuts(occ):
        out = terms(own, late, 4, (sent, 0), (0, last), (at, size), jnp.bfloat16)
        pieces = [turned(out[d - 1], d) for d in range(1, groups)]
        arrived.append((at, size, pieces[0] if groups == 2 else sum(piece.astype(jnp.float32) for piece in pieces)))
        at += size
        sent, total, _ = lax.optimization_barrier((sent, total, out))
    kept = terms(
        own, [[cross], [fore], *late], 2, (total, 0), (last, 1), everything, arrived=arrived[:1], in_hbm=True
    )[0]
    for first, _, sums in arrived[1:-1]:
        kept = settle(kept, first, sums)
    return settle(kept, arrived[-1][0], arrived[-1][2])


def cuts(count):
    return [1, 1, count - 2] if count > 2 else [1] * count


def solution(mesh):
    placed = (P("blk", None, "grp"), P(), P(), P("blk", None, None))
    return jax.shard_map(shards, mesh=mesh, in_specs=placed, out_specs=P("blk", "grp", None), check_vma=False)
```

```python
import functools

import jax
import jax.numpy as jnp
from jax import lax
from jax.experimental import pallas as pl
from jax.experimental.pallas import tpu as pltpu
from jax.sharding import PartitionSpec as P


LAST = (((1,), (1,)), ((), ()))
CHUNK = 512
GRANT = 20 * 2**20
TILE = 16


def flipped(block, bit):
    return lax.ppermute(block, "blk", [(i ^ bit, i) for i in range(lax.axis_size("blk"))])


def sorted_out(block, distance):
    size = lax.axis_size("blk")
    route = [((i - distance if i & 2 else i + distance) % size, i) for i in range(size)]
    return lax.ppermute(block, "blk", route)


def turned(block, distance):
    size = lax.axis_size("grp")
    return lax.ppermute(block, "grp", [(i, (i + distance) % size) for i in range(size)])


def terms_body(names, layout, parts, rows, chunk, adds, carried, scalars, *refs):
    refs = list(refs)
    shifts, occ, nvir = names["shifts"], names["occ"], names["nvir"]
    count = len(layout)
    o = pl.program_id(1) + names["first_occ"]
    left = [refs.pop(0)[0]]
    if parts > 1:
        ahead, rest = refs.pop(0), refs.pop(0)
        left.append(jnp.where((o + scalars[names["turn"]]) % occ < names["per"], ahead[...], rest[...]))
    right = [[[refs.pop(0) for _ in range(parts)] for _ in range(options)] for options in layout]
    flag_ref, col_ref, row_ref = refs.pop(0), refs.pop(0), refs.pop(0)
    base_ref = refs.pop(0) if carried else None
    extra = [refs.pop(0) for _ in adds]
    out_ref, amp_ref, *chosen = refs
    for n, options in enumerate(layout):
        if options > 1:
            @pl.when((pl.program_id(0) == 0) & (pl.program_id(1) == 0))
            def pick():
                for p in range(parts):
                    chosen[p][...] = jnp.where(scalars[names["pick"]] == 0, right[n][0][p][...], right[n][1][p][...])

            right[n] = chosen
        else:
            right[n] = right[n][0]
    width = left[0].shape[1]
    col = col_ref[0]
    lane = lax.broadcasted_iota(jnp.int32, (1, width), 1)
    flags = flag_ref[0:TILE, :].astype(jnp.float32)[0:1]
    for n in range(count):
        step = scalars[names["steps"] + n]
        theirs = right[n][0][rows : rows + TILE, :].astype(jnp.float32)[0:1]
        source = jnp.where(step > 0, theirs, flags)
        for start in range(0, rows, chunk):
            cut = slice(start, start + chunk)
            other = (scalars[names["start"]] + start) // nvir
            place = jnp.where(step > 0, (other * shifts + step - 1) * occ + o, (o * shifts - step - 1) * occ + other)
            weight = jnp.sum(jnp.where(lane == place, source, 0.0), axis=1, keepdims=True)
            coulomb = None
            for p in range(parts):
                piece = lax.dot_general(left[p], right[n][p][cut, :], LAST, preferred_element_type=jnp.float32)
                coulomb = piece if coulomb is None else coulomb + piece
            denom = col + row_ref[n, :, cut]
            amp_ref[:, n * rows + start : n * rows + start + chunk] = (weight * coulomb / denom).astype(jnp.bfloat16)
    for p in range(parts):
        at = pl.ds(pl.multiple_of(scalars[p], 128), width)
        total = base_ref[0, 0, :, at] if carried else None
        for (begin, size), ref in zip(adds, extra):
            inside = (o >= begin) & (o < begin + size)
            total = total + jnp.where(inside, ref[0, :, at].astype(jnp.float32), 0.0)
        for n in range(count):
            piece = jnp.dot(
                amp_ref[:, n * rows : (n + 1) * rows], right[n][p][0:rows, :], preferred_element_type=jnp.float32
            )
            total = piece if total is None else total + piece
        out_ref[0, 0, :, at] = total.astype(out_ref.dtype)


def terms(own, right, first, base, slabs, occs, dtype=jnp.float32, arrived=(), in_hbm=False):
    left, places = own["left"], own["places"]
    parts = own["parts"]
    layout = [len(options) for options in right]
    count = len(layout)
    occ, nvir, width = left[0].shape
    rows = own["rows"]
    naux = width * parts
    slab = nvir // lax.axis_size("grp")
    first_slab, first_occ = slabs[0], occs[0]
    out = (slabs[1], occs[1], slab, naux)
    block = (1, 1, slab, naux)
    per = occ // parts

    def at_slab(j, s):
        return s[places["slab"] + j + first_slab]

    def at_part(taken):
        def at(j, o, s):
            turned_o = (o + first_occ + s[places["turn"]]) % occ - taken * per
            return jnp.clip(turned_o, 0, per - 1) * (nvir // slab) + at_slab(j, s), 0

        return at

    in_specs = [pl.BlockSpec((1, slab, width), lambda j, o, s: (o + first_occ, at_slab(j, s), 0))]
    in_specs += [pl.BlockSpec((slab, width), at_part(taken)) for taken in range(len(left) - 1)]
    pieces = [piece for options in right for option in options for piece in option]
    in_specs += [pl.BlockSpec(memory_space=pltpu.VMEM)] * len(pieces)
    in_specs += [
        pl.BlockSpec(own["flags"].shape, lambda j, o, s: (0, 0)),
        pl.BlockSpec((1, slab, 1), lambda j, o, s: (o + first_occ, at_slab(j, s), 0)),
        pl.BlockSpec((count, 1, rows), lambda j, o, s: (0, 0, 0)),
    ]
    args = [*left, *pieces, own["flags"], own["col"], own["row"][first : first + count]]
    if base is not None:
        skip = first_slab - base[1]
        in_specs.append(pl.BlockSpec(block, lambda j, o, s: (j + skip, o + first_occ, 0, 0)))
        args.append(pltpu.with_memory_space_constraint(base[0], pltpu.HBM))
    for begin, size, sums in arrived:
        in_specs.append(
            pl.BlockSpec(
                (1, slab, naux), lambda j, o, s, b=begin, z=size: (jnp.clip(o + first_occ - b, 0, z - 1), 0, 0)
            )
        )
        args.append(sums)
    moved = sum(piece.size * 2 for piece in pieces) + out[0] * out[1] * slab * naux * 10
    names = {
        "occ": occ, "nvir": nvir, "shifts": own["shifts"], "first_occ": first_occ, "per": per,
        "steps": places["steps"] + first, "start": places["start"], "turn": places["turn"], "pick": places["pick"],
    }
    scratch = [pltpu.VMEM((slab, count * rows), jnp.bfloat16)]
    if max(layout) > 1:
        scratch += [pltpu.VMEM(piece.shape, piece.dtype) for piece in right[layout.index(2)][0]]
    return pl.pallas_call(
        functools.partial(
            terms_body, names, layout, parts, rows, min(CHUNK, rows, nvir), [a[:2] for a in arrived], base is not None
        ),
        grid_spec=pltpu.PrefetchScalarGridSpec(
            num_scalar_prefetch=1,
            grid=(slabs[1], occs[1]),
            in_specs=in_specs,
            out_specs=pl.BlockSpec(block, lambda j, o, s: (j, o, 0, 0)),
            scratch_shapes=scratch,
        ),
        out_shape=pltpu.HBM(out, dtype) if in_hbm else jax.ShapeDtypeStruct(out, dtype),
        compiler_params=pltpu.CompilerParams(
            dimension_semantics=("arbitrary", "arbitrary"), vmem_limit_bytes=GRANT
        ),
        cost_estimate=pl.CostEstimate(
            flops=4 * out[0] * out[1] * slab * rows * count * naux, bytes_accessed=moved, transcendentals=0
        ),
        name="terms",
    )(own["scalars"], *args)


def settle_body(kept_ref, sums_ref, out_ref):
    out_ref[...] = kept_ref[...] + sums_ref[...].astype(jnp.float32)


def settle(kept, first, sums):
    block = (1, *kept.shape[1:])
    return pl.pallas_call(
        settle_body,
        grid=(sums.shape[0],),
        in_specs=[pl.BlockSpec(block, lambda o: (o + first, 0, 0)), pl.BlockSpec(block, lambda o: (o, 0, 0))],
        out_specs=pl.BlockSpec(block, lambda o: (o + first, 0, 0)),
        out_shape=jax.ShapeDtypeStruct(kept.shape, kept.dtype),
        input_output_aliases={0: 0},
        compiler_params=pltpu.CompilerParams(vmem_limit_bytes=GRANT),
        cost_estimate=pl.CostEstimate(flops=sums.size, bytes_accessed=10 * sums.size, transcendentals=0),
        name="settle",
    )(kept, sums)


def shards(integrals, eps_occ, eps_vir, pair_mask):
    occ, nvir, width = integrals.shape
    shifts = pair_mask.shape[1]
    groups = lax.axis_size("grp")
    cycle = lax.axis_size("blk")
    assert shifts == 4 and cycle % 4 == 0
    rank = lax.axis_index("grp")
    place = lax.axis_index("blk")
    core, side = place & 1, (place >> 1) & 1
    every = occ * nvir
    rows = every // groups
    start = rank * rows

    up_core, up_side = 1 - 2 * core, 1 - 2 * side
    diag = -2 * up_side
    steps = [up_core, 2 * up_side, 2 * up_side + up_core, 4 * up_side, -4 * up_side, -3 * up_core, diag, diag + up_core]
    energy = eps_occ.reshape(cycle, occ)
    row = (energy[(place + jnp.stack(steps)) % cycle][:, :, None] - eps_vir).reshape(-1, 1, every)
    row = lax.dynamic_slice_in_dim(row, start, rows, 2)
    col = (energy[place][:, None] - eps_vir)[:, :, None]

    flat = integrals.reshape(every, width)
    if groups == 2 and occ % 2 == 0:
        per = occ // groups
        flags = jnp.pad(pair_mask.astype(integrals.dtype).reshape(1, -1), ((0, TILE - 1), (0, width - pair_mask.size)))
        ahead = turned(lax.dynamic_slice_in_dim(flat, (1 - rank) * rows, rows, 0), 1)
        mine = [jnp.concatenate([lax.dynamic_slice_in_dim(flat, start, rows, 0), flags]), ahead]
        rest = turned(mine[0], 1)
        left = [integrals, ahead, rest]
        parts = 2
        offsets = [rank * width, (1 - rank) * width]
        turn = (groups - rank) * per
    else:
        left = [lax.all_gather(integrals, "grp", axis=2, tiled=True)]
        naux = left[0].shape[2]
        flags = jnp.pad(pair_mask.astype(integrals.dtype).reshape(1, -1), ((0, TILE - 1), (0, naux - pair_mask.size)))
        mine = [jnp.concatenate([lax.dynamic_slice_in_dim(left[0].reshape(every, naux), start, rows, 0), flags])]
        parts = 1
        offsets, turn = [0 * rank], 0 * rank
    slabs = [(rank + 1 + j) % groups for j in range(groups)]
    pick = jnp.where(core == side, 1, 0)
    scalars = jnp.stack([*offsets, turn, pick, start, *slabs, *steps]).astype(jnp.int32)
    places = {"turn": parts, "pick": parts + 1, "start": parts + 2, "slab": parts + 3, "steps": parts + 3 + groups}
    own = {
        "left": left, "flags": flags, "col": col, "row": row, "scalars": scalars, "places": places, "rows": rows,
        "shifts": shifts, "parts": parts,
    }

    def each(pieces, move):
        out = []
        for piece in pieces:
            out.append(move(piece))
        return out

    everything, both = (0, occ), (0, groups)
    last = groups - 1
    near = each(mine, lambda x: flipped(x, 2))
    fore = each(mine, lambda x: sorted_out(x, 4))
    sibling = each(mine, lambda x: flipped(x, 1))
    cross = each(near[:1], lambda x: flipped(x, 1))
    aft = each(mine[:1], lambda x: sorted_out(x, -4))
    across = each(fore[:1], lambda x: flipped(x, 2))
    far_fore = each(fore[:1], lambda x: flipped(x, 1))
    total = terms(own, [[sibling]], 0, None, both, everything, in_hbm=True)
    total, *moved = lax.optimization_barrier((total, *fore[1:], *mine[1:], *near[1:]))
    again, ours, beside = moved[: parts - 1], moved[parts - 1 : 2 * parts - 2], moved[2 * parts - 2 :]
    cross += each(beside, lambda x: flipped(x, 1))
    across += each(again, lambda x: flipped(x, 2))
    aft += each(ours, lambda x: sorted_out(x, -4))
    far_fore += each(again, lambda x: flipped(x, 1))
    sent = terms(own, [[near], [cross], [fore]], 1, (total, 0), (0, last), everything, in_hbm=True)
    sent, total, across[0], aft[0] = lax.optimization_barrier((sent, total, across[0], aft[0]))
    beyond = each(across[: parts - 1], lambda x: flipped(x, 1))
    far_aft = each(aft[: parts - 1], lambda x: flipped(x, 1))
    total = terms(own, [[near], [cross]], 1, (total, 0), (last, 1), everything, in_hbm=True)
    sent, total, across[-1], aft[-1] = lax.optimization_barrier((sent, total, across[-1], aft[-1]))
    beyond += each(across[-1:], lambda x: flipped(x, 1))
    far_aft += each(aft[-1:], lambda x: flipped(x, 1))
    late = [[aft], [far_fore, far_aft], [across], [beyond]]
    arrived = []
    at = 0
    for size in cuts(occ):
        out = terms(own, late, 4, (sent, 0), (0, last), (at, size), jnp.bfloat16)
        pieces = [turned(out[d - 1], d) for d in range(1, groups)]
        arrived.append((at, size, pieces[0] if groups == 2 else sum(piece.astype(jnp.float32) for piece in pieces)))
        at += size
        sent, total, _ = lax.optimization_barrier((sent, total, out))
    kept = terms(own, [[fore], *late], 3, (total, last), (last, 1), everything, arrived=arrived[:1], in_hbm=True)[0]
    for first, _, sums in arrived[1:-1]:
        kept = settle(kept, first, sums)
    return settle(kept, arrived[-1][0], arrived[-1][2])


def cuts(count):
    return [1, 1, count - 2] if count > 2 else [1] * count


def solution(mesh):
    placed = (P("blk", None, "grp"), P(), P(), P("blk", None, None))
    return jax.shard_map(shards, mesh=mesh, in_specs=placed, out_specs=P("blk", "grp", None), check_vma=False)
```

```python
import functools

import jax
import jax.numpy as jnp
from jax import lax
from jax.experimental import pallas as pl
from jax.experimental.pallas import tpu as pltpu
from jax.sharding import PartitionSpec as P


LAST = (((1,), (1,)), ((), ()))
CHUNK = 512
GRANT = 20 * 2**20
TILE = 16


def flipped(block, bit):
    return lax.ppermute(block, "blk", [(i ^ bit, i) for i in range(lax.axis_size("blk"))])


def sorted_out(block, distance):
    size = lax.axis_size("blk")
    route = [((i - distance if i & 2 else i + distance) % size, i) for i in range(size)]
    return lax.ppermute(block, "blk", route)


def turned(block, distance):
    size = lax.axis_size("grp")
    return lax.ppermute(block, "grp", [(i, (i + distance) % size) for i in range(size)])


def terms_body(names, layout, parts, rows, chunk, adds, carried, scalars, *refs):
    refs = list(refs)
    shifts, occ, nvir = names["shifts"], names["occ"], names["nvir"]
    count = len(layout)
    o = pl.program_id(1) + names["first_occ"]
    left = [refs.pop(0)[0]]
    if parts > 1:
        ahead, rest = refs.pop(0), refs.pop(0)
        left.append(jnp.where((o + scalars[names["turn"]]) % occ < names["per"], ahead[...], rest[...]))
    right = [[[refs.pop(0) for _ in range(parts)] for _ in range(options)] for options in layout]
    flag_ref, col_ref, row_ref = refs.pop(0), refs.pop(0), refs.pop(0)
    base_ref = refs.pop(0) if carried else None
    extra = [refs.pop(0) for _ in adds]
    out_ref, amp_ref, *chosen = refs
    for n, options in enumerate(layout):
        if options > 1:
            @pl.when((pl.program_id(0) == 0) & (pl.program_id(1) == 0))
            def pick():
                for p in range(parts):
                    chosen[p][...] = jnp.where(scalars[names["pick"]] == 0, right[n][0][p][...], right[n][1][p][...])

            right[n] = chosen
        else:
            right[n] = right[n][0]
    width = left[0].shape[1]
    col = col_ref[0]
    lane = lax.broadcasted_iota(jnp.int32, (1, width), 1)
    flags = flag_ref[0:TILE, :].astype(jnp.float32)[0:1]
    for n in range(count):
        step = scalars[names["steps"] + n]
        theirs = right[n][0][rows : rows + TILE, :].astype(jnp.float32)[0:1]
        source = jnp.where(step > 0, theirs, flags)
        for start in range(0, rows, chunk):
            cut = slice(start, start + chunk)
            other = (scalars[names["start"]] + start) // nvir
            place = jnp.where(step > 0, (other * shifts + step - 1) * occ + o, (o * shifts - step - 1) * occ + other)
            weight = jnp.sum(jnp.where(lane == place, source, 0.0), axis=1, keepdims=True)
            coulomb = None
            for p in range(parts):
                piece = lax.dot_general(left[p], right[n][p][cut, :], LAST, preferred_element_type=jnp.float32)
                coulomb = piece if coulomb is None else coulomb + piece
            denom = col + row_ref[n, :, cut]
            amp_ref[:, n * rows + start : n * rows + start + chunk] = (weight * coulomb / denom).astype(jnp.bfloat16)
    for p in range(parts):
        at = pl.ds(pl.multiple_of(scalars[p], 128), width)
        total = base_ref[0, 0, :, at] if carried else None
        for (begin, size), ref in zip(adds, extra):
            inside = (o >= begin) & (o < begin + size)
            total = total + jnp.where(inside, ref[0, :, at].astype(jnp.float32), 0.0)
        for n in range(count):
            piece = jnp.dot(
                amp_ref[:, n * rows : (n + 1) * rows], right[n][p][0:rows, :], preferred_element_type=jnp.float32
            )
            total = piece if total is None else total + piece
        out_ref[0, 0, :, at] = total.astype(out_ref.dtype)


def terms(own, right, first, base, slabs, occs, dtype=jnp.float32, arrived=(), in_hbm=False):
    left, places = own["left"], own["places"]
    parts = own["parts"]
    layout = [len(options) for options in right]
    count = len(layout)
    occ, nvir, width = left[0].shape
    rows = own["rows"]
    naux = width * parts
    slab = nvir // lax.axis_size("grp")
    first_slab, first_occ = slabs[0], occs[0]
    out = (slabs[1], occs[1], slab, naux)
    block = (1, 1, slab, naux)
    per = occ // parts

    def at_slab(j, s):
        return s[places["slab"] + j + first_slab]

    def at_part(taken):
        def at(j, o, s):
            turned_o = (o + first_occ + s[places["turn"]]) % occ - taken * per
            return jnp.clip(turned_o, 0, per - 1) * (nvir // slab) + at_slab(j, s), 0

        return at

    in_specs = [pl.BlockSpec((1, slab, width), lambda j, o, s: (o + first_occ, at_slab(j, s), 0))]
    in_specs += [pl.BlockSpec((slab, width), at_part(taken)) for taken in range(len(left) - 1)]
    pieces = [piece for options in right for option in options for piece in option]
    in_specs += [pl.BlockSpec(memory_space=pltpu.VMEM)] * len(pieces)
    in_specs += [
        pl.BlockSpec(own["flags"].shape, lambda j, o, s: (0, 0)),
        pl.BlockSpec((1, slab, 1), lambda j, o, s: (o + first_occ, at_slab(j, s), 0)),
        pl.BlockSpec((count, 1, rows), lambda j, o, s: (0, 0, 0)),
    ]
    args = [*left, *pieces, own["flags"], own["col"], own["row"][first : first + count]]
    if base is not None:
        skip = first_slab - base[1]
        in_specs.append(pl.BlockSpec(block, lambda j, o, s: (j + skip, o + first_occ, 0, 0)))
        args.append(pltpu.with_memory_space_constraint(base[0], pltpu.HBM))
    for begin, size, sums in arrived:
        in_specs.append(
            pl.BlockSpec(
                (1, slab, naux), lambda j, o, s, b=begin, z=size: (jnp.clip(o + first_occ - b, 0, z - 1), 0, 0)
            )
        )
        args.append(sums)
    moved = sum(piece.size * 2 for piece in pieces) + out[0] * out[1] * slab * naux * 10
    names = {
        "occ": occ, "nvir": nvir, "shifts": own["shifts"], "first_occ": first_occ, "per": per,
        "steps": places["steps"] + first, "start": places["start"], "turn": places["turn"], "pick": places["pick"],
    }
    scratch = [pltpu.VMEM((slab, count * rows), jnp.bfloat16)]
    if max(layout) > 1:
        scratch += [pltpu.VMEM(piece.shape, piece.dtype) for piece in right[layout.index(2)][0]]
    return pl.pallas_call(
        functools.partial(
            terms_body, names, layout, parts, rows, min(CHUNK, rows, nvir), [a[:2] for a in arrived], base is not None
        ),
        grid_spec=pltpu.PrefetchScalarGridSpec(
            num_scalar_prefetch=1,
            grid=(slabs[1], occs[1]),
            in_specs=in_specs,
            out_specs=pl.BlockSpec(block, lambda j, o, s: (j, o, 0, 0)),
            scratch_shapes=scratch,
        ),
        out_shape=pltpu.HBM(out, dtype) if in_hbm else jax.ShapeDtypeStruct(out, dtype),
        compiler_params=pltpu.CompilerParams(
            dimension_semantics=("arbitrary", "arbitrary"), vmem_limit_bytes=GRANT
        ),
        cost_estimate=pl.CostEstimate(
            flops=4 * out[0] * out[1] * slab * rows * count * naux, bytes_accessed=moved, transcendentals=0
        ),
        name="terms",
    )(own["scalars"], *args)


def settle_body(kept_ref, sums_ref, out_ref):
    out_ref[...] = kept_ref[...] + sums_ref[...].astype(jnp.float32)


def settle(kept, first, sums):
    block = (1, *kept.shape[1:])
    return pl.pallas_call(
        settle_body,
        grid=(sums.shape[0],),
        in_specs=[pl.BlockSpec(block, lambda o: (o + first, 0, 0)), pl.BlockSpec(block, lambda o: (o, 0, 0))],
        out_specs=pl.BlockSpec(block, lambda o: (o + first, 0, 0)),
        out_shape=jax.ShapeDtypeStruct(kept.shape, kept.dtype),
        input_output_aliases={0: 0},
        compiler_params=pltpu.CompilerParams(vmem_limit_bytes=GRANT),
        cost_estimate=pl.CostEstimate(flops=sums.size, bytes_accessed=10 * sums.size, transcendentals=0),
        name="settle",
    )(kept, sums)


def shards(integrals, eps_occ, eps_vir, pair_mask):
    occ, nvir, width = integrals.shape
    shifts = pair_mask.shape[1]
    groups = lax.axis_size("grp")
    cycle = lax.axis_size("blk")
    assert shifts == 4 and cycle % 4 == 0
    rank = lax.axis_index("grp")
    place = lax.axis_index("blk")
    core, side = place & 1, (place >> 1) & 1
    every = occ * nvir
    rows = every // groups
    start = rank * rows

    up_core, up_side = 1 - 2 * core, 1 - 2 * side
    diag = -2 * up_side
    steps = [up_core, 2 * up_side, 2 * up_side + up_core, 4 * up_side, -4 * up_side, -3 * up_core, diag, diag + up_core]
    energy = eps_occ.reshape(cycle, occ)
    row = (energy[(place + jnp.stack(steps)) % cycle][:, :, None] - eps_vir).reshape(-1, 1, every)
    row = lax.dynamic_slice_in_dim(row, start, rows, 2)
    col = (energy[place][:, None] - eps_vir)[:, :, None]

    flat = integrals.reshape(every, width)
    if groups == 2 and occ % 2 == 0:
        per = occ // groups
        flags = jnp.pad(pair_mask.astype(integrals.dtype).reshape(1, -1), ((0, TILE - 1), (0, width - pair_mask.size)))
        ahead = turned(lax.dynamic_slice_in_dim(flat, (1 - rank) * rows, rows, 0), 1)
        mine = [jnp.concatenate([lax.dynamic_slice_in_dim(flat, start, rows, 0), flags]), ahead]
        rest = turned(mine[0], 1)
        left = [integrals, ahead, rest]
        parts = 2
        offsets = [rank * width, (1 - rank) * width]
        turn = (groups - rank) * per
    else:
        left = [lax.all_gather(integrals, "grp", axis=2, tiled=True)]
        naux = left[0].shape[2]
        flags = jnp.pad(pair_mask.astype(integrals.dtype).reshape(1, -1), ((0, TILE - 1), (0, naux - pair_mask.size)))
        mine = [jnp.concatenate([lax.dynamic_slice_in_dim(left[0].reshape(every, naux), start, rows, 0), flags])]
        parts = 1
        offsets, turn = [0 * rank], 0 * rank
    slabs = [(rank + 1 + j) % groups for j in range(groups)]
    pick = jnp.where(core == side, 1, 0)
    scalars = jnp.stack([*offsets, turn, pick, start, *slabs, *steps]).astype(jnp.int32)
    places = {"turn": parts, "pick": parts + 1, "start": parts + 2, "slab": parts + 3, "steps": parts + 3 + groups}
    own = {
        "left": left, "flags": flags, "col": col, "row": row, "scalars": scalars, "places": places, "rows": rows,
        "shifts": shifts, "parts": parts,
    }

    def each(pieces, move):
        out = []
        for piece in pieces:
            out.append(move(piece))
        return out

    everything, both = (0, occ), (0, groups)
    last = groups - 1
    near = each(mine, lambda x: flipped(x, 2))
    fore = each(mine, lambda x: sorted_out(x, 4))
    sibling = each(mine, lambda x: flipped(x, 1))
    cross = each(near, lambda x: flipped(x, 1))
    aft = each(mine[:1], lambda x: sorted_out(x, -4))
    across = each(fore[:1], lambda x: flipped(x, 2))
    far_fore = each(fore[:1], lambda x: flipped(x, 1))
    total = terms(own, [[sibling], [near]], 0, None, both, everything, in_hbm=True)
    total, *moved, across[0], aft[0] = lax.optimization_barrier((total, *fore[1:], *mine[1:], across[0], aft[0]))
    again, ours = moved[: parts - 1], moved[parts - 1 :]
    across += each(again, lambda x: flipped(x, 2))
    aft += each(ours, lambda x: sorted_out(x, -4))
    far_fore += each(again, lambda x: flipped(x, 1))
    beyond = each(across[: parts - 1], lambda x: flipped(x, 1))
    far_aft = each(aft[: parts - 1], lambda x: flipped(x, 1))
    total = terms(own, [[cross], [fore]], 2, (total, 0), both, everything, in_hbm=True)
    total, across[-1], aft[-1] = lax.optimization_barrier((total, across[-1], aft[-1]))
    sent = total
    beyond += each(across[-1:], lambda x: flipped(x, 1))
    far_aft += each(aft[-1:], lambda x: flipped(x, 1))
    late = [[aft], [far_fore, far_aft], [across], [beyond]]
    arrived = []
    at = 0
    for size in cuts(occ):
        out = terms(own, late, 4, (sent, 0), (0, last), (at, size), jnp.bfloat16)
        pieces = [turned(out[d - 1], d) for d in range(1, groups)]
        arrived.append((at, size, pieces[0] if groups == 2 else sum(piece.astype(jnp.float32) for piece in pieces)))
        at += size
        sent, total, _ = lax.optimization_barrier((sent, total, out))
    kept = terms(own, late, 4, (total, 0), (last, 1), everything, arrived=arrived[:1], in_hbm=True)[0]
    for first, _, sums in arrived[1:-1]:
        kept = settle(kept, first, sums)
    return settle(kept, arrived[-1][0], arrived[-1][2])


def cuts(count):
    return [1, 1, count - 2] if count > 2 else [1] * count


def solution(mesh):
    placed = (P("blk", None, "grp"), P(), P(), P("blk", None, None))
    return jax.shard_map(shards, mesh=mesh, in_specs=placed, out_specs=P("blk", "grp", None), check_vma=False)
```
